32 devices in a mesh: groups: 2 (over y), slab: 4 (over z), pencil: 2 (over x), comp: 2 (over core).
Axes of the slice: x: 2, y: 2, z: 4, core: 2. Of those that a mesh axis runs over, the one named last changes fastest.
Arguments:
- u_start: float32 [3, 64, 64, 512], P(None, ('groups', 'slab'), 'pencil', 'comp'), parts along dimension 1, may hold values from -6 to 6
- toughness: float32 [64, 64, 512], P(('groups', 'slab'), 'pencil', 'comp'), parts along dimension 0, may hold values from 0.3 to 1.5
- crack_label: int32 [64, 64, 512], P(('groups', 'slab'), 'pencil', 'comp'), parts along dimension 0, may hold values from 0 to 2
- obs_weight: bfloat16 [32, 64, 2, 4096], P('slab', 'pencil', 'comp'), may hold values from -0.75 to 0.75
- sensor_cell: int32 [4096], replicated, may hold values from 0 to 4095
Outputs:
- moved: float32 [3, 64, 64, 512], P(None, ('groups', 'slab'), 'pencil', 'comp'), parts along dimension 1
- damage: float32 [64, 64, 512], P(('groups', 'slab'), 'pencil', 'comp'), parts along dimension 0
- readings: float32 [3, 8192], P(None, 'groups'), parts along dimension 1
The draws below stay inside these ranges and needn't reach their ends.
There are 2 independent parts, one for each index of `groups`. The reference program is written for one: setup_inputs(seed, part) draws one part's arguments, and reference() takes and returns one part's arrays. A program takes and returns all parts, laid end to end along the dimension named above; an argument that names none is the same for every part. Nothing has to cross between parts.
Inputs may be any that keep to these rules, and one draw needn't show every extreme that they name: `sensor_cell`: numbers cell blocks as (64 z + y) * 2 + h. `crack_label`: 0 intact, 1 partly cracked, 2 cracked.
All inputs are finite; a program needn't handle non-finite values.
Results may differ from the reference program's by a relative error of at most 0.003.
Values sent between devices are 32-bit elements; how exact they have to be, the bound alone decides.
A program may use at most 128 MiB of HBM per device.

```python
import math
import jax
import jax.numpy as jnp

CX = 256
SENSORS = 4096
NZ = 32
NY = 64
NX = 512
BLOCKS = 4096
N_COMP = 2


def set_ends(array, rng, least, largest):
    longest = array.shape.index(max(array.shape))
    spots = []
    for shift in (0, 1):
        where = [jax.random.randint(jax.random.fold_in(rng, axis), (), 0, length) for axis, length in enumerate(array.shape)]
        where[longest] = (where[longest] + shift) % array.shape[longest]
        spots.append(tuple(where))
    return array.at[spots[0]].set(least).at[spots[1]].set(largest)


def steps_of(key, extent, cuts, low, largest):
    def one(dim, shards_of):
        heights = jax.random.uniform(jax.random.fold_in(jax.random.fold_in(key, 6), dim), (shards_of,), jnp.float32, low / len(cuts), largest / len(cuts))
        return jnp.repeat(jnp.exp(heights), extent[dim] // shards_of).reshape((-1,) + (1,) * (len(extent) - dim - 1))

    gain = one(*cuts[0])
    for cut in cuts[1:]:
        gain = gain * one(*cut)
    return gain


def normal_values(stream_key, extent, width, limit, cuts=(), held_as=jnp.bfloat16):
    loudness = steps_of(stream_key, extent, cuts, -0.22, 0.18) if cuts else 1.0
    array = jax.random.normal(stream_key, extent, jnp.float32) * width * loudness
    return jnp.minimum(jnp.maximum(array, -limit), limit).astype(held_as)


def setup_inputs(seed: int = 0, part: int = 0) -> dict:
    key_list = jax.random.split(jax.random.key(seed), 6)
    part_splits = jax.random.split(jax.random.fold_in(key_list[5], part), 6)
    u_start = normal_values(part_splits[0], (3, NZ, NY, NX), 1.0, 6.0, ((1, 4), (2, 2), (3, 2)), jnp.float32)
    toughness = jnp.clip(jnp.exp(math.log(1.5) - 1.60943787 * jax.random.uniform(part_splits[1], (NZ, NY, NX), jnp.float32) ** steps_of(part_splits[1], (NZ, NY, NX), ((0, 4), (1, 2), (2, 2)), -0.2, 0.2)), 0.3, 1.5)
    crack_label = set_ends(jax.random.randint(part_splits[2], (NZ, NY, NX), 0, 3), jax.random.fold_in(part_splits[2], 1), 0, 2).astype(jnp.int32)
    obs_weight = normal_values(key_list[3], (NZ, NY, N_COMP, SENSORS), (BLOCKS // 64) ** -0.5, 0.75, ((0, 4), (1, 2), (2, 2)))
    sensor_cell = set_ends(jax.random.randint(key_list[4], (SENSORS,), 0, BLOCKS), jax.random.fold_in(key_list[4], 1), 0, BLOCKS - 1).astype(jnp.int32)
    return dict(u_start=u_start, toughness=toughness, crack_label=crack_label, obs_weight=obs_weight, sensor_cell=sensor_cell)


SHEAR_MODULUS = 1.0
LAME_FIRST = 1.5
RESIDUAL_STIFF = 0.001
TIME_DISP = 0.15
TIME_DAMAGE = 0.08
LENGTH_SCALE = 1.0
DAMAGE_LEVEL = 0.45
POINT_GAIN = 8.0


def central(source, spatial):
    if spatial == 0:
        return 0.5 * (source[..., 2:, 1:-1, 1:-1] - source[..., :-2, 1:-1, 1:-1])
    if spatial == 1:
        return 0.5 * (source[..., 1:-1, 2:, 1:-1] - source[..., 1:-1, :-2, 1:-1])
    return 0.5 * (source[..., 1:-1, 1:-1, 2:] - source[..., 1:-1, 1:-1, :-2])


def shrink(source):
    return source[..., 1:-1, 1:-1, 1:-1]


def laplace(source):
    return (source[2:, 1:-1, 1:-1] + source[:-2, 1:-1, 1:-1] + source[1:-1, 2:, 1:-1]
            + source[1:-1, :-2, 1:-1] + source[1:-1, 1:-1, 2:] + source[1:-1, 1:-1, :-2]
            - 6.0 * source[1:-1, 1:-1, 1:-1])


def entry_key(first, second):
    return (min(first, second), max(first, second))


def rotate(matrix, first, second):
    other = 3 - first - second
    diag_first = matrix[(first, first)]
    diag_second = matrix[(second, second)]
    coupling = matrix[(first, second)]
    angle = 0.5 * jnp.arctan2(2.0 * coupling, diag_second - diag_first)
    cosine = jnp.cos(angle)
    sine = jnp.sin(angle)
    side_first = matrix[entry_key(other, first)]
    side_second = matrix[entry_key(other, second)]
    result = dict(matrix)
    result[(first, first)] = cosine * cosine * diag_first - 2.0 * cosine * sine * coupling + sine * sine * diag_second
    result[(second, second)] = sine * sine * diag_first + 2.0 * cosine * sine * coupling + cosine * cosine * diag_second
    result[(first, second)] = jnp.zeros_like(coupling)
    result[entry_key(other, first)] = cosine * side_first - sine * side_second
    result[entry_key(other, second)] = sine * side_first + cosine * side_second
    return result


def eigenvalues(matrix):
    for sweep_index in range(5):
        for first, second in ((0, 1), (0, 2), (1, 2)):
            matrix = rotate(matrix, first, second)
    return [matrix[(0, 0)], matrix[(1, 1)], matrix[(2, 2)]]


def advance(padded_disp, padded_damage, toughness):
    gradient = [[central(padded_disp[component], direction) for direction in range(3)] for component in range(3)]
    strain = {}
    for first in range(3):
        for second in range(first, 3):
            strain[(first, second)] = 0.5 * (gradient[first][second] + gradient[second][first])
    trace_full = strain[(0, 0)] + strain[(1, 1)] + strain[(2, 2)]
    damage_mid = shrink(padded_damage)
    degrade = (1.0 - damage_mid) ** 2 + RESIDUAL_STIFF
    divergence = []
    for component in range(3):
        total_force = 0.0
        for direction in range(3):
            stress = 2.0 * SHEAR_MODULUS * strain[entry_key(component, direction)]
            if component == direction:
                stress = stress + LAME_FIRST * trace_full
            total_force = total_force + central(degrade * stress, direction)
        divergence.append(total_force)
    moved = shrink(shrink(padded_disp)) + TIME_DISP * jnp.stack(divergence)
    inner = {key_pair: shrink(entry_value) for key_pair, entry_value in strain.items()}
    trace_inner = shrink(trace_full)
    energy = 0.5 * LAME_FIRST * jnp.maximum(trace_inner, 0.0) ** 2
    for eigen_value in eigenvalues(inner):
        energy = energy + SHEAR_MODULUS * jnp.maximum(eigen_value, 0.0) ** 2
    damage_core = shrink(damage_mid)
    damage = damage_core + TIME_DAMAGE * (2.0 * (1.0 - damage_core) * energy
                                          - toughness / LENGTH_SCALE * damage_core
                                          + toughness * LENGTH_SCALE * laplace(damage_mid))
    return moved, damage


def reference(u_start, toughness, crack_label, obs_weight, sensor_cell):
    damage = DAMAGE_LEVEL * crack_label.astype(jnp.float32)
    moved = u_start
    for repeat in range(2):
        padded_disp = jnp.pad(moved, ((0, 0), (2, 2), (2, 2), (2, 2)))
        padded_damage = jnp.pad(damage, 2)
        moved, damage = advance(padded_disp, padded_damage, toughness)
    pooled = jnp.mean(moved.reshape(3, NZ, NY, N_COMP, CX), axis=-1)
    pooled = pooled.reshape(3, NZ * NY * N_COMP).astype(jnp.bfloat16)
    dense = jnp.dot(pooled, obs_weight.reshape(NZ * NY * N_COMP, SENSORS), preferred_element_type=jnp.float32)
    point = pooled.astype(jnp.float32)[:, sensor_cell]
    readings = dense + POINT_GAIN * point
    return moved, damage, readings
```

```python
import itertools

import jax
import jax.numpy as jnp
import numpy as np
from jax import lax
from jax.experimental import pallas as pl
from jax.experimental.pallas import tpu as pltpu
from jax.sharding import PartitionSpec as P

RESIDUAL_STIFF = 0.001
TIME_DISP = 0.15
TIME_DAMAGE = 0.08
DAMAGE_LEVEL = 0.45
POINT_GAIN = 8.0
AXES = ("slab", "pencil", "comp")
MESH = pl.DeviceIdType.MESH
F32 = jnp.float32


def third_angle_poly():
    nodes = 0.5 + 0.5 * np.cos(np.pi * (np.arange(200) + 0.5) / 200)
    fit = np.polynomial.chebyshev.Chebyshev.fit(
        nodes, np.cos(np.arccos(nodes) / 3.0), 8, domain=[0.0, 1.0]
    )
    return [float(c) for c in fit.convert(kind=np.polynomial.Polynomial).coef]


POLY = third_angle_poly()

DIRECTIONS = [
    d for d in itertools.product((-1, 0, 1), repeat=3) if 1 <= sum(map(abs, d)) <= 2
]
FAST = [d for d in DIRECTIONS if d[0] == 0]
SLOW = [d for d in DIRECTIONS if d[0] != 0]


def energy_of(e00, e11, e22, e01, e02, e12):
    trace = e00 + e11 + e22
    mean = trace * (1.0 / 3.0)
    d0, d1, d2 = e00 - mean, e11 - mean, e22 - mean
    p2 = (d0 * d0 + d1 * d1 + d2 * d2) * (1.0 / 6.0) + (
        e01 * e01 + e02 * e02 + e12 * e12
    ) * (1.0 / 3.0)
    inv = lax.rsqrt(jnp.maximum(p2, 1e-36))
    p = p2 * inv
    b0, b1, b2 = d0 * inv, d1 * inv, d2 * inv
    b01, b02, b12 = e01 * inv, e02 * inv, e12 * inv
    half_det = 0.5 * (
        b0 * (b1 * b2 - b12 * b12)
        - b01 * (b01 * b2 - b12 * b02)
        + b02 * (b01 * b12 - b1 * b02)
    )
    r = jnp.minimum(jnp.abs(half_det), 1.0)
    c = jnp.full_like(r, POLY[-1])
    for coefficient in POLY[-2::-1]:
        c = c * r + coefficient
    tc = p * c
    t = jnp.where(half_det < 0.0, -tc, tc)
    s2 = jnp.maximum(1.0 - c * c, 0.0)
    delta = p * (s2 * lax.rsqrt(jnp.maximum(s2, 1e-30))) * float(np.sqrt(3.0))
    f1 = jnp.maximum(mean + 2.0 * t, 0.0)
    f2 = jnp.maximum(mean - t + delta, 0.0)
    f3 = jnp.maximum(mean - t - delta, 0.0)
    ft = jnp.maximum(trace, 0.0)
    return 0.75 * ft * ft + f1 * f1 + f2 * f2 + f3 * f3


def make_kernel(planes, rows, columns, sensors, sizes, owners):
    n_slab, n_pencil, n_comp = sizes
    count = n_slab * n_pencil * n_comp
    Z, R, C = planes, rows, columns
    piece = sensors // owners
    half = piece // 2

    def kernel(u_hbm, tough_hbm, crack_hbm, weight_hbm, cell_ref,
               moved_ref, damage_ref, read_ref,
               U, XR, YR, YP, YXR, TZ, tough, crack, weight, pooled_t, hot, partial, RB, GB,
               in_sem, send_sem, recv_sem, rs_send, rs_recv, ag_send, ag_recv):
        me = [lax.axis_index(a) for a in AXES]
        flat = (me[0] * n_pencil + me[1]) * n_comp + me[2]

        def device(index):
            return {
                "slab": index // (n_pencil * n_comp),
                "pencil": (index // n_comp) % n_pencil,
                "comp": index % n_comp,
            }

        loads = [
            pltpu.make_async_copy(u_hbm, U.at[0, 0:3, 2:Z + 2, 0:R, 0:C], in_sem.at[0]),
            pltpu.make_async_copy(crack_hbm, crack, in_sem.at[1]),
            pltpu.make_async_copy(tough_hbm, tough, in_sem.at[2]),
            pltpu.make_async_copy(weight_hbm, weight, in_sem.at[3]),
        ]
        for load in loads:
            load.start()

        for step in range(2):
            for z in (0, 1, Z + 2, Z + 3):
                U[step, :, z, 0:R, 0:C] = jnp.zeros((4, R, C), F32)
        XR[...] = jnp.zeros(XR.shape, F32)
        YR[...] = jnp.zeros(YR.shape, F32)
        YXR[...] = jnp.zeros(YXR.shape, F32)

        barrier = pltpu.get_barrier_semaphore()

        def greet(k, carry):
            pl.semaphore_signal(
                barrier, inc=1, device_id=device((flat + k) % count), device_id_type=MESH
            )
            return carry

        lax.fori_loop(1, count, greet, 0)
        pl.semaphore_wait(barrier, count - 1)

        loads[1].wait()

        def label(z, carry):
            U[0, 3, z + 2, 0:R, 0:C] = DAMAGE_LEVEL * crack[z].astype(F32)
            return carry

        lax.fori_loop(0, Z, label, 0)
        loads[0].wait()

        def copies(step, d):
            dz, dy, dx = d
            sy, sx = (dy + 1) // 2, (dx + 1) // 2
            lanes = slice(C - 128, C) if dx > 0 else slice(0, 128)
            edge = Z - 1 if dz > 0 else 0
            halo = 0 if dz > 0 else Z + 1
            if dz and not dy and not dx:
                first = Z if dz > 0 else 2
                target = 0 if dz > 0 else Z + 2
                pairs = [
                    (U.at[step, 0:3, first:first + 2, 0:R, 0:C],
                     U.at[step, 0:3, target:target + 2, 0:R, 0:C]),
                    (U.at[step, 3, edge + 2, 0:R, 0:C], U.at[step, 3, halo + 1, 0:R, 0:C]),
                ]
            elif dz and dy:
                pairs = [(YP.at[step, sy, edge], YR.at[step, 1 - sy, halo])]
            elif dz and dx:
                pairs = [(U.at[step, 0:3, edge + 2, 0:R, lanes], XR.at[step, 1 - sx, 0:3, halo])]
            elif dy and dx:
                pairs = [(YP.at[step, sy, :, :, lanes], YXR.at[step, 1 - sy, 1 - sx])]
            elif dy:
                pairs = [(YP.at[step, sy], YR.at[step, 1 - sy, 1:Z + 1])]
            else:
                pairs = [(U.at[step, :, 2:Z + 2, 0:R, lanes], XR.at[step, 1 - sx, :, 1:Z + 1])]
            index = DIRECTIONS.index(d)
            return [
                pltpu.make_async_remote_copy(
                    src_ref=src,
                    dst_ref=dst,
                    send_sem=send_sem.at[step, index, k],
                    recv_sem=recv_sem.at[step, index, k],
                    device_id={a: m + o for a, m, o in zip(AXES, me, d)},
                    device_id_type=MESH,
                )
                for k, (src, dst) in enumerate(pairs)
            ]

        def inside(d, sign):
            ok = None
            for m, o, n in zip(me, d, sizes):
                if o:
                    here = m + 1 < n if sign * o > 0 else m >= 1
                    ok = here if ok is None else jnp.logical_and(ok, here)
            return ok

        def feasible(d):
            return all(n > 1 for o, n in zip(d, sizes) if o)

        def each(step, directions, sign, action):
            for d in directions:
                if feasible(d):
                    @pl.when(inside(d, sign))
                    def _():
                        for copy in copies(step, d):
                            action(copy)

        row8 = lax.broadcasted_iota(jnp.int32, (8, C), 0)
        row8t = lax.broadcasted_iota(jnp.int32, (8, 128), 0)
        lane8 = lax.broadcasted_iota(jnp.int32, (8, 128), 1)
        lane_r = lax.broadcasted_iota(jnp.int32, (R, 128), 1)

        def roll(value, shift, axis):
            shift = shift % value.shape[axis]
            return pltpu.roll(value, shift, axis) if shift else value

        def pack(step):
            def one(z, carry):
                low = [U[step, f, z + 2, 0:8, 0:C] for f in range(4)]
                high = [U[step, f, z + 2, R - 8:R, 0:C] for f in range(4)]
                for side, tiles, shifts in (
                    (0, low, (0, 2, 4, 6)), (1, high, (2, 4, 6, 7))
                ):
                    rolled = [roll(t, s, 0) for t, s in zip(tiles, shifts)]
                    YP[step, side, z] = jnp.where(
                        row8 < 2, rolled[0],
                        jnp.where(row8 < 4, rolled[1], jnp.where(row8 < 6, rolled[2], rolled[3])),
                    )
                return carry

            lax.fori_loop(0, Z, one, 0)

        def merged(low, high, f, row):
            up, down = ((8 - 2 * f) % 8, 6 - 2 * f) if f < 3 else (2, 1)
            return jnp.where(row < 4, roll(high, up, 0), roll(low, down, 0))

        def unpack(step, z, full):
            fields = range(4 if full else 3)
            low, high = YR[step, 0, z + 1], YR[step, 1, z + 1]
            for f in fields:
                U[step, f, z + 2, R:R + 8, 0:C] = merged(low, high, f, row8)
                U[step, f, z + 2, 0:R, C:C + 128] = jnp.where(
                    lane_r < 64, XR[step, 1, f, z + 1], XR[step, 0, f, z + 1]
                )
            if full:
                left, right = [
                    [YXR[step, sy, sx, z] for sy in range(2)] for sx in range(2)
                ]
                for f in range(3):
                    U[step, f, z + 2, R:R + 8, C:C + 128] = jnp.where(
                        lane8 < 64, merged(*right, f, row8t), merged(*left, f, row8t)
                    )

        def ends(step, z):
            now = [U[step, i, z + 2] for i in range(3)]
            gz = [
                U[step, i, z + 3, 0:R, 0:C] - U[step, i, z + 1, 0:R, 0:C] for i in range(3)
            ]

            def along(value, axis):
                return (roll(value, -1, axis) - roll(value, 1, axis))[0:R, 0:C]

            gy0, gy1 = along(now[0], 0), along(now[1], 0)
            gx0, gx2 = along(now[0], 1), along(now[2], 1)
            keep = 1.0 - U[step, 3, z + 2, 0:R, 0:C]
            g = (0.5 * TIME_DISP) * (keep * keep + RESIDUAL_STIFF)
            TZ[z + 1, 0] = g * (gz[0] + 0.75 * (gz[0] + gy1 + gx2))
            TZ[z + 1, 1] = g * (0.5 * (gz[1] + gy0))
            TZ[z + 1, 2] = g * (0.5 * (gz[2] + gx0))

        def store(step, f, z, value):
            if step == 0:
                U[1, f, z + 2, 0:R, 0:C] = value
            elif f < 3:
                moved_ref[f, z] = value
            else:
                damage_ref[z] = value

        def load(step, f, z):
            return U[1, f, z + 2, 0:R, 0:C] if step == 0 else moved_ref[f, z]

        def body(step, z):
            now = [U[step, i, z + 2] for i in range(3)]
            gz = [U[step, i, z + 3] - U[step, i, z + 1] for i in range(3)]
            gy = [roll(v, -1, 0) - roll(v, 1, 0) for v in now]
            gx = [roll(v, -1, 1) - roll(v, 1, 1) for v in now]
            d = U[step, 3, z + 2]
            keep = 1.0 - d
            g = (0.5 * TIME_DISP) * (keep * keep + RESIDUAL_STIFF)
            lam = 0.75 * (gz[0] + gy[1] + gx[2])
            s01 = 0.5 * (gz[1] + gy[0])
            s02 = 0.5 * (gz[2] + gx[0])
            s12 = 0.5 * (gy[2] + gx[1])
            in_y = [g * s01, g * (gy[1] + lam), g * s12]
            in_x = [(g * s02)[0:R], in_y[2][0:R], (g * (gx[2] + lam))[0:R]]
            TZ[z + 1, 0] = (g * (gz[0] + lam))[0:R, 0:C]
            TZ[z + 1, 1] = in_y[0][0:R, 0:C]
            TZ[z + 1, 2] = in_x[0][:, 0:C]
            for i in range(3):
                ty = in_y[i][:, 0:C]
                force = (roll(ty, -1, 0) - roll(ty, 1, 0))[0:R] + (
                    roll(in_x[i], -1, 1) - roll(in_x[i], 1, 1)
                )[:, 0:C]
                store(step, i, z, now[i][0:R, 0:C] + force)

            def core(value):
                return value[0:R, 0:C]

            energy = energy_of(
                0.5 * core(gz[0]), 0.5 * core(gy[1]), 0.5 * core(gx[2]),
                0.5 * core(s01), 0.5 * core(s02), 0.5 * core(s12),
            )
            dy = d[:, 0:C]
            dx = d[0:R]
            dc = core(d)
            lap = (
                U[step, 3, z + 3, 0:R, 0:C] + U[step, 3, z + 1, 0:R, 0:C]
                + (roll(dy, -1, 0) + roll(dy, 1, 0))[0:R]
                + (roll(dx, -1, 1) + roll(dx, 1, 1))[:, 0:C]
                - 6.0 * dc
            )
            store(step, 3, z, dc + TIME_DAMAGE * (
                2.0 * (1.0 - dc) * energy + tough[z] * (lap - dc)
            ))

        def finish(step, z):
            for i in range(3):
                store(step, i, z, load(step, i, z) + (TZ[z + 2, i] - TZ[z, i]))

        def loop(start, stop, function):
            def one(z, carry):
                function(z)
                return carry

            lax.fori_loop(start, stop, one, 0)

        for step in range(2):
            pack(step)
            each(step, SLOW, 1, lambda copy: copy.start())
            each(step, FAST, 1, lambda copy: copy.start())
            if step == 0:
                loads[2].wait()
                base = me[0] * Z * (R * n_pencil) + me[1] * R
                row_id = lax.broadcasted_iota(jnp.int32, (R, 512), 0) * n_comp

                def choose(z, carry):
                    start = (base + z * (R * n_pencil)) * n_comp + me[2]
                    for s in range(0, sensors, 512):
                        hit = row_id == cell_ref[:, s:s + 512] - start
                        hot[z, :, s:s + 512] = jnp.where(hit, POINT_GAIN, 0.0).astype(jnp.bfloat16)
                    return carry

                lax.fori_loop(0, Z, choose, 0)
            each(step, FAST, -1, lambda copy: copy.wait_recv())
            loop(0, Z, lambda z: unpack(step, z, True))
            loop(1, Z - 1, lambda z: body(step, z))
            each(step, SLOW, -1, lambda copy: copy.wait_recv())
            unpack(step, -1, False)
            unpack(step, Z, False)
            loop(0, 2, lambda k: body(step, k * (Z - 1)))
            loop(0, 2, lambda k: ends(step, k * (Z + 1) - 1))
            loop(0, Z, lambda z: finish(step, z))
            each(step, SLOW, 1, lambda copy: copy.wait_send())
            each(step, FAST, 1, lambda copy: copy.wait_send())

        def pool(z):
            total = jnp.zeros((R, 128), F32)
            for i in range(3):
                mean = jnp.sum(moved_ref[i, z], axis=1, keepdims=True) * (1.0 / C)
                total = jnp.where(lane_r == i, mean, total)
            pooled_t[pl.ds(pl.multiple_of(z * R, R), R), :] = total

        loop(0, Z, pool)
        pooled = pooled_t[...].T[0:8].astype(jnp.bfloat16)
        loads[3].wait()
        chunk = piece
        for q in range(owners):
            for h in range(2):
                s = q * piece + h * half
                value = jnp.dot(
                    pooled, weight[:, s:s + half], preferred_element_type=F32
                ) + jnp.dot(
                    pooled, hot[:, :, s:s + half].reshape(Z * R, half), preferred_element_type=F32
                )
                partial[q, 4 * h:4 * h + 4] = value[0:4]

        def scatter(q):
            return pltpu.make_async_remote_copy(
                src_ref=partial.at[q], dst_ref=RB.at[flat],
                send_sem=rs_send.at[q], recv_sem=rs_recv.at[flat],
                device_id=device(q), device_id_type=MESH,
            )

        def scatter_from(k):
            return pltpu.make_async_remote_copy(
                src_ref=partial.at[0], dst_ref=RB.at[k],
                send_sem=rs_send.at[0], recv_sem=rs_recv.at[k],
                device_id=device(k), device_id_type=MESH,
            )

        def gather(q, k):
            return pltpu.make_async_remote_copy(
                src_ref=GB.at[q], dst_ref=GB.at[q],
                send_sem=ag_send.at[k], recv_sem=ag_recv.at[q],
                device_id=device(k), device_id_type=MESH,
            )

        def others(stop, function):
            def one(k):
                @pl.when(k != flat)
                def _():
                    function(k)

            loop(0, stop, one)

        others(owners, lambda q: scatter(q).start())

        @pl.when(flat < owners)
        def _():
            others(count, lambda k: scatter_from(k).wait_recv())
            RB[flat] = partial[flat]

            def add(k, total):
                return total + RB[k]

            GB[flat] = lax.fori_loop(1, count, add, RB[0])
            others(count, lambda k: gather(flat, k).start())

        others(owners, lambda q: gather(q, 0).wait_recv())
        for q in range(owners):
            read_ref[:, q * piece:q * piece + half] = GB[q, 0:3]
            read_ref[:, q * piece + half:(q + 1) * piece] = GB[q, 4:7]
        others(owners, lambda q: scatter(q).wait_send())

        @pl.when(flat < owners)
        def _():
            others(count, lambda k: gather(flat, k).wait_send())

    return kernel


def solution(mesh):
    sizes = tuple(mesh.shape[a] for a in AXES)
    count = sizes[0] * sizes[1] * sizes[2]

    def local(u_start, toughness, crack_label, obs_weight, sensor_cell):
        Z, R, C = toughness.shape
        S = sensor_cell.shape[0]
        owners = 1
        while owners * 2 <= count and S % (owners * 512) == 0:
            owners *= 2
        piece = S // owners
        n_dir = len(DIRECTIONS)
        any_spec = pl.BlockSpec(memory_space=pl.ANY)
        vmem_spec = pl.BlockSpec(memory_space=pltpu.VMEM)
        dma = pltpu.SemaphoreType.DMA
        return pl.pallas_call(
            make_kernel(Z, R, C, S, sizes, owners),
            out_shape=(
                jax.ShapeDtypeStruct((3, Z, R, C), F32),
                jax.ShapeDtypeStruct((Z, R, C), F32),
                jax.ShapeDtypeStruct((3, S), F32),
            ),
            in_specs=[any_spec] * 4 + [vmem_spec],
            out_specs=[vmem_spec] * 3,
            scratch_shapes=[
                pltpu.VMEM((2, 4, Z + 4, R + 8, C + 128), F32),
                pltpu.VMEM((2, 2, 4, Z + 2, R, 128), F32),
                pltpu.VMEM((2, 2, Z + 2, 8, C), F32),
                pltpu.VMEM((2, 2, Z, 8, C), F32),
                pltpu.VMEM((2, 2, 2, Z, 8, 128), F32),
                pltpu.VMEM((Z + 2, 3, R, C), F32),
                pltpu.VMEM((Z, R, C), F32),
                pltpu.VMEM((Z, R, C), jnp.int32),
                pltpu.VMEM((Z * R, S), jnp.bfloat16),
                pltpu.VMEM((Z * R, 128), F32),
                pltpu.VMEM((Z, R, S), jnp.bfloat16),
                pltpu.VMEM((owners, 8, piece // 2), F32),
                pltpu.VMEM((count, 8, piece // 2), F32),
                pltpu.VMEM((owners, 8, piece // 2), F32),
                dma((4,)),
                dma((2, n_dir, 2)),
                dma((2, n_dir, 2)),
                dma((owners,)),
                dma((count,)),
                dma((count,)),
                dma((owners,)),
            ],
            compiler_params=pltpu.CompilerParams(
                collective_id=0, has_side_effects=True, vmem_limit_bytes=60 * 1024 * 1024
            ),
            name="fracture",
        )(
            u_start, toughness, crack_label,
            obs_weight.reshape(Z * R, S), sensor_cell.reshape(1, S),
        )

    return jax.shard_map(
        local,
        mesh=mesh,
        in_specs=(
            P(None, ("groups", "slab"), "pencil", "comp"),
            P(("groups", "slab"), "pencil", "comp"),
            P(("groups", "slab"), "pencil", "comp"),
            P("slab", "pencil", "comp", None),
            P(),
        ),
        out_specs=(
            P(None, ("groups", "slab"), "pencil", "comp"),
            P(("groups", "slab"), "pencil", "comp"),
            P(None, "groups"),
        ),
        check_vma=False,
    )
```

```python
import itertools

import jax
import jax.numpy as jnp
import numpy as np
from jax import lax
from jax.experimental import pallas as pl
from jax.experimental.pallas import tpu as pltpu
from jax.sharding import PartitionSpec as P

RESIDUAL_STIFF = 0.001
TIME_DISP = 0.15
TIME_DAMAGE = 0.08
DAMAGE_LEVEL = 0.45
POINT_GAIN = 8.0
AXES = ("slab", "pencil", "comp")
MESH = pl.DeviceIdType.MESH
F32 = jnp.float32


def third_angle_poly():
    nodes = 0.5 + 0.5 * np.cos(np.pi * (np.arange(200) + 0.5) / 200)
    fit = np.polynomial.chebyshev.Chebyshev.fit(
        nodes, np.cos(np.arccos(nodes) / 3.0), 8, domain=[0.0, 1.0]
    )
    return [float(c) for c in fit.convert(kind=np.polynomial.Polynomial).coef]


POLY = third_angle_poly()

DIRECTIONS = [
    d for d in itertools.product((-1, 0, 1), repeat=3) if 1 <= sum(map(abs, d)) <= 2
]
FAST_X = [d for d in DIRECTIONS if d[0] == 0 and d[1] == 0]
FAST_Y = [d for d in DIRECTIONS if d[0] == 0 and d[1] != 0]
FACES = [(0, 0, -1), (0, 0, 1), (-1, 0, 0), (1, 0, 0), (0, -1, 0), (0, 1, 0)]
ORDER = FACES + [d for d in FAST_Y if d[2]] + [d for d in DIRECTIONS if d[0] and (d[1] or d[2])]
SLOW = [d for d in DIRECTIONS if d[0] != 0]


def energy_of(e00, e11, e22, e01, e02, e12):
    trace = e00 + e11 + e22
    mean = trace * (1.0 / 3.0)
    d0, d1, d2 = e00 - mean, e11 - mean, e22 - mean
    p2 = (d0 * d0 + d1 * d1 + d2 * d2) * (1.0 / 6.0) + (
        e01 * e01 + e02 * e02 + e12 * e12
    ) * (1.0 / 3.0)
    inv = lax.rsqrt(jnp.maximum(p2, 1e-36))
    p = p2 * inv
    b0, b1, b2 = d0 * inv, d1 * inv, d2 * inv
    b01, b02, b12 = e01 * inv, e02 * inv, e12 * inv
    half_det = 0.5 * (
        b0 * (b1 * b2 - b12 * b12)
        - b01 * (b01 * b2 - b12 * b02)
        + b02 * (b01 * b12 - b1 * b02)
    )
    r = jnp.minimum(jnp.abs(half_det), 1.0)
    c = jnp.full_like(r, POLY[-1])
    for coefficient in POLY[-2::-1]:
        c = c * r + coefficient
    tc = p * c
    t = jnp.where(half_det < 0.0, -tc, tc)
    s2 = jnp.maximum(1.0 - c * c, 0.0)
    delta = p * (s2 * lax.rsqrt(jnp.maximum(s2, 1e-30))) * float(np.sqrt(3.0))
    f1 = jnp.maximum(mean + 2.0 * t, 0.0)
    f2 = jnp.maximum(mean - t + delta, 0.0)
    f3 = jnp.maximum(mean - t - delta, 0.0)
    ft = jnp.maximum(trace, 0.0)
    return 0.75 * ft * ft + f1 * f1 + f2 * f2 + f3 * f3


def make_kernel(planes, rows, columns, sensors, sizes, owners):
    n_slab, n_pencil, n_comp = sizes
    count = n_slab * n_pencil * n_comp
    Z, R, C = planes, rows, columns
    piece = sensors // owners
    half = piece // 2

    def kernel(u_hbm, tough_hbm, crack_hbm, weight_hbm, cell_ref,
               moved_ref, damage_ref, read_ref,
               U, XR, YR, YP, YXR, TZ, tough, crack, weight, pooled_t, hot, partial, RB, GB,
               in_sem, send_sem, recv_sem, rs_send, rs_recv, ag_send, ag_recv):
        me = [lax.axis_index(a) for a in AXES]
        flat = (me[0] * n_pencil + me[1]) * n_comp + me[2]

        def device(index):
            return {
                "slab": index // (n_pencil * n_comp),
                "pencil": (index // n_comp) % n_pencil,
                "comp": index % n_comp,
            }

        loads = [
            pltpu.make_async_copy(u_hbm, U.at[0, 0:3, 2:Z + 2, 0:R, 0:C], in_sem.at[0]),
            pltpu.make_async_copy(crack_hbm, crack, in_sem.at[1]),
            pltpu.make_async_copy(tough_hbm, tough, in_sem.at[2]),
            pltpu.make_async_copy(weight_hbm, weight, in_sem.at[3]),
        ]
        for load in loads:
            load.start()

        for step in range(2):
            for z in (0, 1, Z + 2, Z + 3):
                U[step, :, z, 0:R, 0:C] = jnp.zeros((4, R, C), F32)
        XR[...] = jnp.zeros(XR.shape, F32)
        YR[...] = jnp.zeros(YR.shape, F32)
        YXR[...] = jnp.zeros(YXR.shape, F32)

        barrier = pltpu.get_barrier_semaphore()

        def greet(k, carry):
            pl.semaphore_signal(
                barrier, inc=1, device_id=device((flat + k) % count), device_id_type=MESH
            )
            return carry

        lax.fori_loop(1, count, greet, 0)
        pl.semaphore_wait(barrier, count - 1)

        loads[1].wait()

        def label(z, carry):
            U[0, 3, z + 2, 0:R, 0:C] = DAMAGE_LEVEL * crack[z].astype(F32)
            return carry

        lax.fori_loop(0, Z, label, 0)
        loads[0].wait()

        def copies(step, d):
            dz, dy, dx = d
            sy, sx = (dy + 1) // 2, (dx + 1) // 2
            lanes = slice(C - 128, C) if dx > 0 else slice(0, 128)
            edge = Z - 1 if dz > 0 else 0
            halo = 0 if dz > 0 else Z + 1
            if dz and not dy and not dx:
                first = Z if dz > 0 else 2
                target = 0 if dz > 0 else Z + 2
                pairs = [
                    (U.at[step, 0:3, first:first + 2, 0:R, 0:C],
                     U.at[step, 0:3, target:target + 2, 0:R, 0:C]),
                    (U.at[step, 3, edge + 2, 0:R, 0:C], U.at[step, 3, halo + 1, 0:R, 0:C]),
                ]
            elif dz and dy:
                pairs = [(YP.at[step, sy, edge], YR.at[step, 1 - sy, halo])]
            elif dz and dx:
                pairs = [(U.at[step, 0:3, edge + 2, 0:R, lanes], XR.at[step, 1 - sx, 0:3, halo])]
            elif dy and dx:
                pairs = [(YP.at[step, sy, :, :, lanes], YXR.at[step, 1 - sy, 1 - sx])]
            elif dy:
                pairs = [(YP.at[step, sy], YR.at[step, 1 - sy, 1:Z + 1])]
            else:
                pairs = [(U.at[step, :, 2:Z + 2, 0:R, lanes], XR.at[step, 1 - sx, :, 1:Z + 1])]
            index = DIRECTIONS.index(d)
            return [
                pltpu.make_async_remote_copy(
                    src_ref=src,
                    dst_ref=dst,
                    send_sem=send_sem.at[step, index, k],
                    recv_sem=recv_sem.at[step, index, k],
                    device_id={a: m + o for a, m, o in zip(AXES, me, d)},
                    device_id_type=MESH,
                )
                for k, (src, dst) in enumerate(pairs)
            ]

        def inside(d, sign):
            ok = None
            for m, o, n in zip(me, d, sizes):
                if o:
                    here = m + 1 < n if sign * o > 0 else m >= 1
                    ok = here if ok is None else jnp.logical_and(ok, here)
            return ok

        def feasible(d):
            return all(n > 1 for o, n in zip(d, sizes) if o)

        def each(step, directions, sign, action):
            for d in directions:
                if feasible(d):
                    @pl.when(inside(d, sign))
                    def _():
                        for copy in copies(step, d):
                            action(copy)

        row8 = lax.broadcasted_iota(jnp.int32, (8, C), 0)
        row8t = lax.broadcasted_iota(jnp.int32, (8, 128), 0)
        lane8 = lax.broadcasted_iota(jnp.int32, (8, 128), 1)
        lane_r = lax.broadcasted_iota(jnp.int32, (R, 128), 1)

        def roll(value, shift, axis):
            shift = shift % value.shape[axis]
            return pltpu.roll(value, shift, axis) if shift else value

        def pack(step):
            def one(z, carry):
                low = [U[step, f, z + 2, 0:8, 0:C] for f in range(4)]
                high = [U[step, f, z + 2, R - 8:R, 0:C] for f in range(4)]
                for side, tiles, shifts in (
                    (0, low, (0, 2, 4, 6)), (1, high, (2, 4, 6, 7))
                ):
                    rolled = [roll(t, s, 0) for t, s in zip(tiles, shifts)]
                    YP[step, side, z] = jnp.where(
                        row8 < 2, rolled[0],
                        jnp.where(row8 < 4, rolled[1], jnp.where(row8 < 6, rolled[2], rolled[3])),
                    )
                return carry

            lax.fori_loop(0, Z, one, 0)

        def merged(low, high, f, row):
            up, down = ((8 - 2 * f) % 8, 6 - 2 * f) if f < 3 else (2, 1)
            return jnp.where(row < 4, roll(high, up, 0), roll(low, down, 0))

        def unpack_x(step, z, fields):
            for f in range(fields):
                U[step, f, z + 2, 0:R, C:C + 128] = jnp.where(
                    lane_r < 64, XR[step, 1, f, z + 1], XR[step, 0, f, z + 1]
                )

        def unpack_y(step, z, fields):
            low, high = YR[step, 0, z + 1], YR[step, 1, z + 1]
            for f in range(fields):
                U[step, f, z + 2, R:R + 8, 0:C] = merged(low, high, f, row8)
            if fields == 4:
                left, right = [
                    [YXR[step, sy, sx, z] for sy in range(2)] for sx in range(2)
                ]
                for f in range(3):
                    U[step, f, z + 2, R:R + 8, C:C + 128] = jnp.where(
                        lane8 < 64, merged(*right, f, row8t), merged(*left, f, row8t)
                    )

        def ends(step, z):
            now = [U[step, i, z + 2] for i in range(3)]
            gz = [
                U[step, i, z + 3, 0:R, 0:C] - U[step, i, z + 1, 0:R, 0:C] for i in range(3)
            ]

            def along(value, axis):
                return (roll(value, -1, axis) - roll(value, 1, axis))[0:R, 0:C]

            gy0, gy1 = along(now[0], 0), along(now[1], 0)
            gx0, gx2 = along(now[0], 1), along(now[2], 1)
            keep = 1.0 - U[step, 3, z + 2, 0:R, 0:C]
            g = (0.5 * TIME_DISP) * (keep * keep + RESIDUAL_STIFF)
            TZ[z + 1, 0] = g * (gz[0] + 0.75 * (gz[0] + gy1 + gx2))
            TZ[z + 1, 1] = g * (0.5 * (gz[1] + gy0))
            TZ[z + 1, 2] = g * (0.5 * (gz[2] + gx0))

        def store(step, f, z, value):
            if step == 0:
                U[1, f, z + 2, 0:R, 0:C] = value
            elif f < 3:
                moved_ref[f, z] = value
            else:
                damage_ref[z] = value

        def load(step, f, z):
            return U[1, f, z + 2, 0:R, 0:C] if step == 0 else moved_ref[f, z]

        def body(step, z):
            now = [U[step, i, z + 2] for i in range(3)]
            gz = [U[step, i, z + 3] - U[step, i, z + 1] for i in range(3)]
            gy = [roll(v, -1, 0) - roll(v, 1, 0) for v in now]
            gx = [roll(v, -1, 1) - roll(v, 1, 1) for v in now]
            d = U[step, 3, z + 2]
            keep = 1.0 - d
            g = (0.5 * TIME_DISP) * (keep * keep + RESIDUAL_STIFF)
            lam = 0.75 * (gz[0] + gy[1] + gx[2])
            s01 = 0.5 * (gz[1] + gy[0])
            s02 = 0.5 * (gz[2] + gx[0])
            s12 = 0.5 * (gy[2] + gx[1])
            in_y = [g * s01, g * (gy[1] + lam), g * s12]
            in_x = [(g * s02)[0:R], in_y[2][0:R], (g * (gx[2] + lam))[0:R]]
            TZ[z + 1, 0] = (g * (gz[0] + lam))[0:R, 0:C]
            TZ[z + 1, 1] = in_y[0][0:R, 0:C]
            TZ[z + 1, 2] = in_x[0][:, 0:C]
            for i in range(3):
                ty = in_y[i][:, 0:C]
                force = (roll(ty, -1, 0) - roll(ty, 1, 0))[0:R] + (
                    roll(in_x[i], -1, 1) - roll(in_x[i], 1, 1)
                )[:, 0:C]
                store(step, i, z, now[i][0:R, 0:C] + force)

            def core(value):
                return value[0:R, 0:C]

            energy = energy_of(
                0.5 * core(gz[0]), 0.5 * core(gy[1]), 0.5 * core(gx[2]),
                0.5 * core(s01), 0.5 * core(s02), 0.5 * core(s12),
            )
            dy = d[:, 0:C]
            dx = d[0:R]
            dc = core(d)
            lap = (
                U[step, 3, z + 3, 0:R, 0:C] + U[step, 3, z + 1, 0:R, 0:C]
                + (roll(dy, -1, 0) + roll(dy, 1, 0))[0:R]
                + (roll(dx, -1, 1) + roll(dx, 1, 1))[:, 0:C]
                - 6.0 * dc
            )
            store(step, 3, z, dc + TIME_DAMAGE * (
                2.0 * (1.0 - dc) * energy + tough[z] * (lap - dc)
            ))

        def finish(step, z):
            for i in range(3):
                store(step, i, z, load(step, i, z) + (TZ[z + 2, i] - TZ[z, i]))

        def loop(start, stop, function):
            def one(z, carry):
                function(z)
                return carry

            lax.fori_loop(start, stop, one, 0)

        for step in range(2):
            pack(step)
            each(step, ORDER, 1, lambda copy: copy.start())
            if step == 0:
                loads[2].wait()
                base = me[0] * Z * (R * n_pencil) + me[1] * R
                row_id = lax.broadcasted_iota(jnp.int32, (R, 512), 0) * n_comp

                def choose(z, carry):
                    start = (base + z * (R * n_pencil)) * n_comp + me[2]
                    for s in range(0, sensors, 512):
                        hit = row_id == cell_ref[:, s:s + 512] - start
                        hot[z, :, s:s + 512] = jnp.where(hit, POINT_GAIN, 0.0).astype(jnp.bfloat16)
                    return carry

                lax.fori_loop(0, Z, choose, 0)
            each(step, FAST_X, -1, lambda copy: copy.wait_recv())
            loop(0, Z, lambda z: unpack_x(step, z, 4))
            each(step, FAST_Y, -1, lambda copy: copy.wait_recv())
            loop(0, Z, lambda z: unpack_y(step, z, 4))
            loop(1, Z - 1, lambda z: body(step, z))
            each(step, SLOW, -1, lambda copy: copy.wait_recv())
            for z in (-1, Z):
                unpack_x(step, z, 3)
                unpack_y(step, z, 3)
            loop(0, 2, lambda k: body(step, k * (Z - 1)))
            loop(0, 2, lambda k: ends(step, k * (Z + 1) - 1))
            loop(0, Z, lambda z: finish(step, z))
            each(step, ORDER, 1, lambda copy: copy.wait_send())

        def pool(z):
            total = jnp.zeros((R, 128), F32)
            for i in range(3):
                mean = jnp.sum(moved_ref[i, z], axis=1, keepdims=True) * (1.0 / C)
                total = jnp.where(lane_r == i, mean, total)
            pooled_t[pl.ds(pl.multiple_of(z * R, R), R), :] = total

        loop(0, Z, pool)
        pooled = pooled_t[...].T[0:8].astype(jnp.bfloat16)
        loads[3].wait()
        def scatter(q):
            return pltpu.make_async_remote_copy(
                src_ref=partial.at[q], dst_ref=RB.at[flat],
                send_sem=rs_send.at[q], recv_sem=rs_recv.at[flat],
                device_id=device(q), device_id_type=MESH,
            )

        def scatter_from(k):
            return pltpu.make_async_remote_copy(
                src_ref=partial.at[0], dst_ref=RB.at[k],
                send_sem=rs_send.at[0], recv_sem=rs_recv.at[k],
                device_id=device(k), device_id_type=MESH,
            )

        def gather(q, k):
            return pltpu.make_async_remote_copy(
                src_ref=GB.at[q], dst_ref=GB.at[q],
                send_sem=ag_send.at[k], recv_sem=ag_recv.at[q],
                device_id=device(k), device_id_type=MESH,
            )

        def others(stop, function):
            def one(k):
                @pl.when(k != flat)
                def _():
                    function(k)

            loop(0, stop, one)

        for q in range(owners):
            for h in range(2):
                cut = q * piece + h * half
                value = jnp.dot(
                    pooled, weight[:, cut:cut + half], preferred_element_type=F32
                ) + jnp.dot(
                    pooled, hot[:, :, cut:cut + half].reshape(Z * R, half),
                    preferred_element_type=F32,
                )
                partial[q, 4 * h:4 * h + 4] = value[0:4]

        def send(k):
            q = (flat + k) % count

            @pl.when(q < owners)
            def _():
                scatter(q).start()

        loop(1, count, send)

        @pl.when(flat < owners)
        def _():
            others(count, lambda k: scatter_from(k).wait_recv())
            RB[flat] = partial[flat]

            def add(k, total):
                return total + RB[k]

            GB[flat] = lax.fori_loop(1, count, add, RB[0])
            loop(1, count, lambda k: gather(flat, (flat + k) % count).start())

        others(owners, lambda q: gather(q, 0).wait_recv())
        for q in range(owners):
            read_ref[:, q * piece:q * piece + half] = GB[q, 0:3]
            read_ref[:, q * piece + half:(q + 1) * piece] = GB[q, 4:7]
        others(owners, lambda q: scatter(q).wait_send())

        @pl.when(flat < owners)
        def _():
            others(count, lambda k: gather(flat, k).wait_send())

    return kernel


def solution(mesh):
    sizes = tuple(mesh.shape[a] for a in AXES)
    count = sizes[0] * sizes[1] * sizes[2]

    def local(u_start, toughness, crack_label, obs_weight, sensor_cell):
        Z, R, C = toughness.shape
        S = sensor_cell.shape[0]
        owners = 1
        while owners * 2 <= count and S % (owners * 512) == 0:
            owners *= 2
        piece = S // owners
        n_dir = len(DIRECTIONS)
        any_spec = pl.BlockSpec(memory_space=pltpu.HBM)
        vmem_spec = pl.BlockSpec(memory_space=pltpu.VMEM)
        dma = pltpu.SemaphoreType.DMA
        return pl.pallas_call(
            make_kernel(Z, R, C, S, sizes, owners),
            out_shape=(
                jax.ShapeDtypeStruct((3, Z, R, C), F32),
                jax.ShapeDtypeStruct((Z, R, C), F32),
                jax.ShapeDtypeStruct((3, S), F32),
            ),
            in_specs=[any_spec] * 4 + [vmem_spec],
            out_specs=[vmem_spec] * 3,
            scratch_shapes=[
                pltpu.VMEM((2, 4, Z + 4, R + 8, C + 128), F32),
                pltpu.VMEM((2, 2, 4, Z + 2, R, 128), F32),
                pltpu.VMEM((2, 2, Z + 2, 8, C), F32),
                pltpu.VMEM((2, 2, Z, 8, C), F32),
                pltpu.VMEM((2, 2, 2, Z, 8, 128), F32),
                pltpu.VMEM((Z + 2, 3, R, C), F32),
                pltpu.VMEM((Z, R, C), F32),
                pltpu.VMEM((Z, R, C), jnp.int32),
                pltpu.VMEM((Z * R, S), jnp.bfloat16),
                pltpu.VMEM((Z * R, 128), F32),
                pltpu.VMEM((Z, R, S), jnp.bfloat16),
                pltpu.VMEM((owners, 8, piece // 2), F32),
                pltpu.VMEM((count, 8, piece // 2), F32),
                pltpu.VMEM((owners, 8, piece // 2), F32),
                dma((4,)),
                dma((2, n_dir, 2)),
                dma((2, n_dir, 2)),
                dma((owners,)),
                dma((count,)),
                dma((count,)),
                dma((owners,)),
            ],
            compiler_params=pltpu.CompilerParams(
                collective_id=0, has_side_effects=True, vmem_limit_bytes=40 * 1024 * 1024
            ),
            name="fracture",
        )(
            *[
                pltpu.with_memory_space_constraint(x, pltpu.HBM)
                for x in (u_start, toughness, crack_label, obs_weight.reshape(Z * R, S))
            ],
            sensor_cell.reshape(1, S),
        )

    return jax.shard_map(
        local,
        mesh=mesh,
        in_specs=(
            P(None, ("groups", "slab"), "pencil", "comp"),
            P(("groups", "slab"), "pencil", "comp"),
            P(("groups", "slab"), "pencil", "comp"),
            P("slab", "pencil", "comp", None),
            P(),
        ),
        out_specs=(
            P(None, ("groups", "slab"), "pencil", "comp"),
            P(("groups", "slab"), "pencil", "comp"),
            P(None, "groups"),
        ),
        check_vma=False,
    )
```
